32 devices in a mesh: lat: 8 (over z, y), chan: 4 (over x, core).
Axes of the slice: x: 2, y: 2, z: 4, core: 2. Of those that a mesh axis runs over, the one named last changes fastest.
Arguments:
- grid_in: bfloat16 [256, 384, 1024], P('chan', 'lat'), may hold values from -6 to 6
- quad_weights: float32 [384], P('lat'), may hold values from 0.5 to 2
- legendre: bfloat16 [384, 384, 384], P('lat'), as said below
- mixing: bfloat16 [2, 384, 256, 256], P(None, 'lat', 'chan'), may hold values from -0.375 to 0.375
Outputs:
- grid_out: bfloat16 [256, 384, 1024], P('chan', 'lat')
The draws below stay inside these ranges and needn't reach their ends.
Inputs may be any that keep to these rules, and one draw needn't show every extreme that they name: legendre[m, l, t] is zero wherever l < m.
All inputs are finite; a program needn't handle non-finite values.
Results may differ from the reference program's by a relative error of at most 0.0068.
Values may be sent and summed in bfloat16 or wider, within the bound.
A program may use at most 128 MiB of HBM per device.

```python
import math
import jax
import jax.numpy as jnp
from jax import lax

C = 256
NLAT = 384
NLON = 1024
M = 384
L = 384


def draw_legendre(key, part):
    values = jax.random.normal(key, (M, L, NLAT), jnp.float32)
    orders = jnp.arange(M, dtype=jnp.int32)[:, None, None]
    degrees = jnp.arange(L, dtype=jnp.int32)[None, :, None]
    values = jnp.where(degrees >= orders, values, 0.0) * NLAT ** (-0.5)
    return values.astype(jnp.bfloat16)


def spiked(array, own_key, source, target, parts, factor):
    def block_of(axis_at):
        return (jnp.arange(array.shape[axis_at]) // (array.shape[axis_at] // parts)).reshape((-1,) + (1,) * (array.ndim - 1 - axis_at))

    one_side = jax.random.permutation(own_key, parts)[block_of(target)]
    second = (block_of(target) + parts // 2) % parts
    return jnp.where((block_of(source) == one_side) | (block_of(source) == second), factor * array, array)


def levels(rng, dims, pieces, smallest, largest):
    gain = 1.0
    for dim, shards_of in pieces:
        heights = jax.random.uniform(jax.random.fold_in(jax.random.fold_in(rng, 6), dim), (shards_of,), jnp.float32, smallest / len(pieces), largest / len(pieces))
        gain = gain * jnp.repeat(jnp.exp(heights), dims[dim] // shards_of).reshape((-1,) + (1,) * (len(dims) - 1 - dim))
    return gain


def gaussian(stream_key, extent, scale, limit, split=(), held_as=jnp.bfloat16):
    factor_of = levels(stream_key, extent, split, -0.22, 0.18) if split else 1.0
    drawn = jax.random.normal(stream_key, extent, jnp.float32) * scale * factor_of
    return jnp.minimum(jnp.maximum(drawn, -limit), limit).astype(held_as)


def noise_with(own_key, extent, scale, reach, cuts, heavy, kind=jnp.bfloat16):
    array = scale * jax.random.normal(own_key, extent, jnp.float32)
    if cuts:
        array = array * levels(own_key, extent, cuts, -0.22, 0.18)
    return jnp.clip(spiked(array, jax.random.fold_in(own_key, 3), *heavy), -reach, reach).astype(kind)


def setup_inputs(seed: int = 0) -> dict:
    arg_keys = jax.random.split(jax.random.key(seed), 5)
    grid_in = gaussian(arg_keys[0], (C, NLAT, NLON), 1.0, 6.0, ((0, 4), (1, 8)))
    quad_weights = jnp.clip(jnp.exp(math.log(2.0) - 1.3862944 * jax.random.uniform(arg_keys[1], (NLAT,), jnp.float32) ** levels(arg_keys[1], (NLAT,), ((0, 8),), -0.2, 0.2)), 0.5, 2.0)
    legendre = draw_legendre(jax.random.fold_in(arg_keys[4], 71), 0)
    mixing = noise_with(arg_keys[3], (2, L, C, C), (2 * C) ** -0.5, 0.375, ((1, 8), (2, 4)), (2, 3, 4, 2.0))
    return {"grid_in": grid_in, "quad_weights": quad_weights, "legendre": legendre, "mixing": mixing}


def fourier_table(number, length):
    orders = jnp.arange(number, dtype=jnp.int32)
    points = jnp.arange(length, dtype=jnp.int32)
    phases = orders[:, None] * points[None, :] % length
    angles = phases.astype(jnp.float32) * (2.0 * math.pi / length)
    factor = 1.0 / math.sqrt(length)
    return jnp.stack([jnp.cos(angles) * factor, -jnp.sin(angles) * factor]).astype(jnp.bfloat16)

def reference(grid_in, quad_weights, legendre, mixing):
    fourier = fourier_table(M, NLON)
    flattened = grid_in.reshape(C * NLAT, NLON)
    spectra = jnp.dot(flattened, fourier.reshape(2 * M, NLON).T, preferred_element_type=jnp.float32)
    spectra = spectra.reshape(C, NLAT, 2, M) * quad_weights[None, :, None, None]
    weighted = spectra.astype(jnp.bfloat16).transpose(3, 1, 2, 0).reshape(M, NLAT, 2 * C)

    def forward_one(operands):
        return jnp.dot(operands[0], operands[1], preferred_element_type=jnp.float32).astype(jnp.bfloat16)
    coeffs = lax.map(forward_one, (legendre, weighted))
    by_degree = coeffs.transpose(1, 0, 2)
    weights_by = mixing.transpose(1, 0, 2, 3)

    def mix_one(operands):
        values, weight = operands
        real_in = values[:, :C]
        imag_in = values[:, C:]
        real_out = jnp.dot(real_in, weight[0], preferred_element_type=jnp.float32) - jnp.dot(imag_in, weight[1], preferred_element_type=jnp.float32)
        imag_out = jnp.dot(imag_in, weight[0], preferred_element_type=jnp.float32) + jnp.dot(real_in, weight[1], preferred_element_type=jnp.float32)
        return jnp.concatenate([real_out, imag_out], axis=1).astype(jnp.bfloat16)
    mixed_coef = lax.map(mix_one, (by_degree, weights_by)).transpose(1, 0, 2)

    def inverse_one(operands):
        return jnp.dot(operands[0].T, operands[1], preferred_element_type=jnp.float32).astype(jnp.bfloat16)
    synthesis = lax.map(inverse_one, (legendre, mixed_coef))
    spread = synthesis.reshape(M, NLAT, 2, C).transpose(3, 1, 2, 0).reshape(C * NLAT, 2 * M)
    restored = jnp.dot(spread, fourier.reshape(2 * M, NLON), preferred_element_type=jnp.float32)
    return (restored.reshape(C, NLAT, NLON) + grid_in.astype(jnp.float32)).astype(jnp.bfloat16)
```

```python
import functools
import math

import jax
import jax.numpy as jnp
from jax import lax
from jax.experimental import pallas as pl
from jax.sharding import PartitionSpec as P

M = 384
PIECES = (2, 1)


def fourier_table(number, length):
    orders = jnp.arange(number, dtype=jnp.int32)
    points = jnp.arange(length, dtype=jnp.int32)
    phases = orders[:, None] * points[None, :] % length
    angles = phases.astype(jnp.float32) * (2.0 * math.pi / length)
    factor = 1.0 / math.sqrt(length)
    return jnp.stack([jnp.cos(angles) * factor, -jnp.sin(angles) * factor]).astype(jnp.bfloat16)


def step_of(part):
    return next(count for count in (4, 3, 2, 1) if part % count == 0)


def price(legendre, columns):
    orders, degrees, points = legendre.shape
    return pl.CostEstimate(
        flops=2 * orders * degrees * points * columns,
        bytes_accessed=2 * orders * (degrees * points + (degrees + points) * columns),
        transcendentals=0,
    )


def analyse(legendre, gathered, chans):
    lats, orders, rows_lat, columns = gathered.shape
    degrees = legendre.shape[1] // lats
    part = orders // chans
    step = step_of(part)
    runs = part // step

    def kernel(table_ref, values_ref, out_ref):
        for at in range(step):
            values = values_ref[:, at].reshape(lats * rows_lat, columns)
            sums = jnp.dot(table_ref[at], values, preferred_element_type=jnp.float32)
            out_ref[:, 0, at] = sums.astype(jnp.bfloat16).reshape(lats, degrees, columns)

    return pl.pallas_call(
        kernel,
        grid=(orders // step,),
        in_specs=[
            pl.BlockSpec((step,) + legendre.shape[1:], lambda g: (g, 0, 0)),
            pl.BlockSpec((lats, step, rows_lat, columns), lambda g: (0, g, 0, 0)),
        ],
        out_specs=pl.BlockSpec(
            (lats, 1, step, degrees, columns), lambda g: (0, g // runs, g % runs, 0, 0)
        ),
        out_shape=jax.ShapeDtypeStruct((lats, chans, part, degrees, columns), jnp.bfloat16),
        cost_estimate=price(legendre, columns),
    )(legendre, gathered)


def synthesise(legendre, returned, rows_lat):
    lats, chans, part, degrees, columns = returned.shape
    orders = legendre.shape[0]
    step = step_of(part)
    runs = part // step

    def kernel(table_ref, values_ref, out_ref):
        for at in range(step):
            values = values_ref[:, 0, at].reshape(lats * degrees, columns)
            sums = lax.dot_general(
                table_ref[at],
                values,
                (((0,), (0,)), ((), ())),
                preferred_element_type=jnp.float32,
            )
            out_ref[:, at] = sums.astype(jnp.bfloat16).reshape(lats, rows_lat, columns)

    return pl.pallas_call(
        kernel,
        grid=(orders // step,),
        in_specs=[
            pl.BlockSpec((step,) + legendre.shape[1:], lambda g: (g, 0, 0)),
            pl.BlockSpec(
                (lats, 1, step, degrees, columns), lambda g: (0, g // runs, g % runs, 0, 0)
            ),
        ],
        out_specs=pl.BlockSpec((lats, step, rows_lat, columns), lambda g: (0, g, 0, 0)),
        out_shape=jax.ShapeDtypeStruct((lats, orders, rows_lat, columns), jnp.bfloat16),
        cost_estimate=price(legendre, columns),
    )(legendre, returned)


def body(chans, grid_in, quad_weights, legendre, mixing):
    groups = grid_in.shape[0]
    rows_lat = grid_in.shape[1]
    length = grid_in.shape[2]
    orders = legendre.shape[0]
    degrees = mixing.shape[1]
    lats = legendre.shape[1] // degrees
    part = -(-orders // chans)
    padding = part * chans - orders
    everyone = ("lat", "chan")

    channel = jnp.arange(chans * groups)
    place = channel // groups * (2 * groups) + channel % groups
    column = jnp.arange(2 * chans * groups)
    to_real = (column == place[:, None]).astype(jnp.bfloat16)
    to_imag = (column == place[:, None] + groups).astype(jnp.bfloat16)

    def spread_out(table):
        return jnp.einsum(
            "rlcd,rdy->lcy", mixing, table, preferred_element_type=jnp.float32
        ).astype(jnp.bfloat16)

    blocks = jnp.concatenate(
        [
            spread_out(jnp.stack([to_real, to_imag])),
            spread_out(jnp.stack([to_imag, -to_real])),
        ],
        axis=1,
    )
    weights = lax.all_gather(blocks, "chan", axis=0)
    fourier = fourier_table(M, length)
    spectra = jnp.einsum("ctn,rmn->mtrc", grid_in, fourier, preferred_element_type=jnp.float32)
    spectra = spectra * quad_weights[None, :, None, None]
    weighted = spectra.astype(jnp.bfloat16).reshape(M, rows_lat, 2 * groups)
    gathered = lax.all_to_all(weighted, "lat", split_axis=0, concat_axis=0, tiled=True)
    gathered = gathered.reshape(lats, orders, rows_lat, 2 * groups)
    fits = padding == 0 and rows_lat % 16 == 0 and degrees % 16 == 0
    if fits:
        outgoing = analyse(legendre, gathered, chans)
    else:
        whole = gathered.transpose(1, 0, 2, 3).reshape(orders, lats * rows_lat, 2 * groups)
        coeffs = jnp.einsum(
            "mlt,mtk->mlk", legendre, whole, preferred_element_type=jnp.float32
        ).astype(jnp.bfloat16)
        coeffs = jnp.pad(coeffs, ((0, padding), (0, 0), (0, 0)))
        outgoing = coeffs.reshape(chans, part, lats, degrees, 2 * groups)
        outgoing = outgoing.transpose(2, 0, 1, 3, 4)
    pieces = next(count for count in PIECES if part % count == 0)
    width = part // pieces
    place_lat = lax.axis_index("lat")
    peers = jnp.arange(lats).reshape(lats, 1, 1, 1, 1)

    def exchange(buffer, axes):
        flat = buffer.reshape((-1,) + buffer.shape[-3:])
        flat = lax.all_to_all(flat, axes, split_axis=0, concat_axis=0, tiled=True)
        return flat.reshape(buffer.shape)

    def mix(arrived):
        mixed = jnp.einsum(
            "ikmlx,klxy->limy", arrived, weights, preferred_element_type=jnp.float32
        ).astype(jnp.bfloat16)
        mixed = mixed.reshape(degrees, lats, width, chans, 2 * groups)
        return mixed.transpose(1, 3, 2, 0, 4)

    received = [exchange(outgoing[:, :, :width], ("lat", "chan"))]
    own = []
    for piece in range(1, pieces + 1):
        mixed = mix(received[-1])
        if piece < pieces:
            own.append(lax.dynamic_index_in_dim(mixed, place_lat, 0, keepdims=False))
            coming = outgoing[:, :, piece * width : (piece + 1) * width]
            mixed = jnp.where(peers >= place_lat, coming, mixed)
        received.append(exchange(mixed, ("lat", "chan")))
    if own:
        own = exchange(jnp.concatenate(own, axis=1), "chan")
    returned = []
    for piece in range(pieces):
        block = received[piece + 1]
        if piece < pieces - 1:
            mine = own[None, :, piece * width : (piece + 1) * width]
            block = jnp.where(peers == place_lat, mine, block)
        returned.append(jnp.where(peers >= place_lat, block, jnp.zeros_like(block)))
    returned = jnp.concatenate(returned, axis=2)
    if fits:
        synthesis = synthesise(legendre, returned, rows_lat)
    else:
        mixed_coef = returned.transpose(1, 2, 0, 3, 4)
        mixed_coef = mixed_coef.reshape(chans * part, lats * degrees, 2 * groups)[:orders]
        synthesis = jnp.einsum(
            "mlt,mlk->mtk", legendre, mixed_coef, preferred_element_type=jnp.float32
        ).astype(jnp.bfloat16)
        synthesis = synthesis.reshape(orders, lats, rows_lat, 2 * groups).transpose(1, 0, 2, 3)
    synthesis = synthesis.reshape(lats * orders, rows_lat, 2 * groups)
    gridded = lax.all_to_all(synthesis, "lat", split_axis=0, concat_axis=0, tiled=True)
    spread = gridded.reshape(M, rows_lat, 2, groups)
    restored = jnp.einsum("mtrc,rmn->ctn", spread, fourier, preferred_element_type=jnp.float32)
    return (restored + grid_in.astype(jnp.float32)).astype(jnp.bfloat16)


def solution(mesh):
    return jax.shard_map(
        functools.partial(body, mesh.shape["chan"]),
        mesh=mesh,
        in_specs=(
            P("chan", "lat", None),
            P("lat"),
            P("lat", None, None),
            P(None, "lat", "chan", None),
        ),
        out_specs=P("chan", "lat", None),
        check_vma=False,
    )
```
